32 devices in a mesh: rep: 4 (over y, x), feat: 8 (over z, core).
Axes of the slice: x: 2, y: 2, z: 4, core: 2. Of those that a mesh axis runs over, the one named last changes fastest.
Arguments:
- basis: float32 [4, 64, 32768], P('rep', None, 'feat'), may hold values from -6 to 6
- stream: bfloat16 [4, 2, 128, 32768], P('rep', None, None, 'feat'), may hold values from -6 to 6
Outputs:
- new_basis: float32 [4, 64, 32768], P('rep', None, 'feat')
The draws below stay inside these ranges and needn't reach their ends.
All inputs are finite; a program needn't handle non-finite values.
Results may differ from the reference program's by a relative error of at most 0.0003.
Values sent between devices are 32-bit elements; how exact they have to be, the bound alone decides.
A program may use at most 64 MiB of HBM per device.

```python
import jax
import jax.numpy as jnp
from jax import lax

RANK = 64
BATCH = 128
STEPS = 2
NF = 32768
REPS = 4


def draw_basis(key, part):
    shape = (REPS, RANK, NF)
    inner = jax.random.fold_in(key, 11)
    values = jax.random.normal(inner, shape, jnp.float32)
    return jnp.clip(values, -6.0, 6.0)


def draw_stream(key, part):
    shape = (REPS, STEPS, BATCH, NF)
    inner = jax.random.fold_in(key, 21)
    values = jax.random.normal(inner, shape, jnp.float32)
    return jnp.clip(values, -6.0, 6.0).astype(jnp.bfloat16)


def setup_inputs(seed: int = 0) -> dict:
    arg_keys = jax.random.split(jax.random.key(seed), 3)
    return {
        "basis": draw_basis(jax.random.fold_in(arg_keys[2], 71), 0),
        "stream": draw_stream(jax.random.fold_in(arg_keys[2], 71), 0),
    }


learn_rate = 0.5

def one_replica(pair):
    start, batches, average = pair
    scale = jnp.sqrt(jnp.float32(NF))
    step_size = learn_rate / BATCH
    current = start
    for step in range(STEPS):
        rows = batches[step].astype(jnp.float32)
        proj = jnp.dot(rows.astype(jnp.float32), current.T.astype(jnp.float32), precision=lax.Precision.HIGHEST, preferred_element_type=jnp.float32) / scale
        cov = jnp.dot(proj.T.astype(jnp.float32), proj.astype(jnp.float32), precision=lax.Precision.HIGHEST, preferred_element_type=jnp.float32)
        drive = jnp.dot(proj.T.astype(jnp.float32), rows.astype(jnp.float32), precision=lax.Precision.HIGHEST, preferred_element_type=jnp.float32)
        shrink = jnp.dot(cov.astype(jnp.float32), current.astype(jnp.float32), precision=lax.Precision.HIGHEST, preferred_element_type=jnp.float32)
        current = current + step_size * (drive - shrink)
    mixed = current + average - start
    gram = jnp.dot(mixed.astype(jnp.float32), mixed.T.astype(jnp.float32), precision=lax.Precision.HIGHEST, preferred_element_type=jnp.float32) / NF
    lower = jnp.linalg.cholesky(gram)
    return lax.linalg.triangular_solve(lower, mixed, left_side=True, lower=True)

def reference(basis, stream):
    average = lax.optimization_barrier(jnp.sum(basis, axis=0)) / REPS

    def apply_one(pair):
        return one_replica((pair[0], pair[1], average))
    return lax.map(apply_one, (basis, stream))
```

```python
import functools

import jax
import jax.numpy as jnp
from jax import lax
from jax.experimental import pallas as pl
from jax.experimental.pallas import tpu as pltpu
from jax.sharding import PartitionSpec as P

learn_rate = 0.5
LANE = 128
MESH = pl.DeviceIdType.MESH
NN = (((1,), (0,)), ((), ()))
NT = (((1,), (1,)), ((), ()))


def exact_dot(left, right, dims):
    return lax.dot_general(
        left, right, dims, precision=lax.Precision.HIGHEST, preferred_element_type=jnp.float32
    )


def fast_dot(left, right, dims):
    return lax.dot_general(left, right, dims, preferred_element_type=jnp.float32)


def halves(value):
    high = value.astype(jnp.bfloat16)
    low = (value - high.astype(jnp.float32)).astype(jnp.bfloat16)
    return high, low


def gather_kernel(
    reps, feats, rank, rows, cols, total_feat,
    basis_hbm, stream_hbm, gram_ref, mixed_hbm,
    w_ref, x_ref, whl_ref, sums_refs, recv_refs, av_ref, m_ref,
    pay_ref, half_recv, half_sum, z_recv, full_ref,
    g_ref, g_core, g_sum, g_recv,
    load_sem, out_sem, ring_send, ring_recv, core_send, core_recv, z_send, z_recv_sem,
    gz_send, gz_recv,
):
    bits = reps.bit_length() - 1
    chunk = LANE * reps
    chunks = cols // chunk
    zs = feats // 2
    me = lax.axis_index("rep")
    feat = lax.axis_index("feat")
    core = feat % 2
    zpos = feat // 2
    eta = learn_rate / rows
    scale = jnp.sqrt(jnp.float32(total_feat))

    load_w = pltpu.make_async_copy(basis_hbm, w_ref, load_sem.at[0])
    load_w.start()
    load_x = pltpu.make_async_copy(stream_hbm, x_ref, load_sem.at[1])
    load_x.start()

    def rep_peer(b):
        bit = (me // (1 << b)) % 2
        return me + (1 - 2 * bit) * (1 << b), bit

    rep_ids = [(rep_peer(b)[0], feat) for b in range(bits)]
    core_id = (me, feat + 1 - 2 * core)
    z_ids = [(me, ((zpos + d) % zs) * 2 + core) for d in range(1, zs)]

    barrier = pltpu.get_barrier_semaphore()
    for peer in rep_ids + [core_id] + z_ids:
        pl.semaphore_signal(barrier, inc=1, device_id=peer, device_id_type=MESH)
    pl.semaphore_wait(barrier, bits + 1 + zs - 1)
    load_w.wait()

    def remote(src, dst, send_sem, recv_sem, peer):
        copy = pltpu.make_async_remote_copy(
            src_ref=src, dst_ref=dst, send_sem=send_sem, recv_sem=recv_sem,
            device_id=peer, device_id_type=MESH,
        )
        copy.start()
        return copy

    started = []

    def at(off, width):
        return pl.ds(pl.multiple_of(off, LANE), width)

    def order(c):
        return [(c + i) % bits for i in range(bits)]

    keeps = []
    for c in range(chunks):
        off = c * chunk
        rec = []
        for i, b in enumerate(order(c)):
            width = chunk >> (i + 1)
            bit = rep_peer(b)[1]
            off = off + bit * width
            rec.append(off)
        keeps.append(rec)

    ring = {}

    def send_scatter(c, i):
        b = order(c)[i]
        width = chunk >> (i + 1)
        bit = rep_peer(b)[1]
        other = (1 - bit) * width
        if i == 0:
            src = w_ref.at[:, at(c * chunk + other, width)]
        else:
            src = sums_refs[i - 1].at[:, at(c * 2 * width + other, width)]
        dst = recv_refs[i].at[:, c * width:(c + 1) * width]
        ring[c, i] = remote(src, dst, ring_send.at[i, c], ring_recv.at[i, c], rep_ids[b])

    def take_scatter(c, i):
        b = order(c)[i]
        width = chunk >> (i + 1)
        bit = rep_peer(b)[1]
        ring[c, i].wait_recv()
        if i == 0:
            own = w_ref[:, at(c * chunk + bit * width, width)]
        else:
            own = sums_refs[i - 1][:, at(c * 2 * width + bit * width, width)]
        total = own + recv_refs[i][:, c * width:(c + 1) * width]
        if i == bits - 1:
            av_ref[:, at(keeps[c][i], width)] = total / reps
        else:
            sums_refs[i][:, c * width:(c + 1) * width] = total

    def send_gather(c, i):
        s = bits - 1 - i
        b = order(c)[s]
        width = chunk >> (s + 1)
        piece = av_ref.at[:, at(keeps[c][s], width)]
        k = bits + i
        ring[c, k] = remote(piece, piece, ring_send.at[k, c], ring_recv.at[k, c], rep_ids[b])

    for c in range(chunks):
        send_scatter(c, 0)

    def step(c, i):
        if i < bits:
            take_scatter(c, i)
        else:
            ring[c, i].wait_recv()
        if i + 1 < bits:
            send_scatter(c, i + 1)
        elif i + 1 < 2 * bits:
            send_gather(c, i + 1 - bits)

    pending = [(c, i) for i in range(2 * bits - 1) for c in range(chunks)]
    place = [0]

    def advance(count):
        for _ in range(count):
            if place[0] < len(pending):
                step(*pending[place[0]])
                place[0] += 1

    high, low = halves(w_ref[...])
    whl_ref[0:rank, :] = high
    whl_ref[rank:2 * rank, :] = low
    load_x.wait()
    x_all = x_ref[...]
    wx = fast_dot(whl_ref[...], x_all, NT)
    wx = wx[0:rank] + wx[rank:2 * rank]
    pay_ref[0:rank, :] = wx[:, 0:rows]
    pay_ref[rank:2 * rank, :] = wx[:, rows:2 * rows]
    pay_ref[2 * rank:2 * rank + rows, :] = fast_dot(x_ref[0:rows, :], x_ref[rows:2 * rows, :], NT)

    half = rank + rows // 2
    give = pl.ds(pl.multiple_of((1 - core) * half, 8), half)
    keep = pl.ds(pl.multiple_of(core * half, 8), half)
    core_copy = remote(pay_ref.at[give, :], half_recv, core_send.at[0], core_recv.at[0], core_id)
    advance(chunks // 4)
    core_copy.wait_recv()
    half_sum[...] = pay_ref[keep, :] + half_recv[...]
    z_copies = [
        remote(half_sum, z_recv.at[d], z_send.at[d], z_recv_sem.at[d], z_ids[d])
        for d in range(zs - 1)
    ]
    started.append(core_copy)
    started.extend(z_copies)
    advance(chunks - chunks // 4 + chunks // 2)
    total = half_sum[...]
    for d in range(zs - 1):
        z_copies[d].wait_recv()
        total = total + z_recv[d]
    full_ref[keep, :] = total
    share = remote(full_ref.at[keep, :], full_ref.at[keep, :], core_send.at[1], core_recv.at[1], core_id)
    started.append(share)
    advance(chunks // 2)
    share.wait_recv()

    first = full_ref[0:rank, :]
    second = full_ref[rank:2 * rank, :]
    cross = full_ref[2 * rank:2 * rank + rows, :]
    proj0 = first / scale
    cov0 = exact_dot(proj0, proj0, NT)
    drive1 = exact_dot(proj0, cross, NN)
    proj1 = (second + eta * (drive1 - exact_dot(cov0, second, NN))) / scale
    cov1 = exact_dot(proj1, proj1, NT)
    advance(chunks // 2)
    k_w = eta * (eta * exact_dot(cov1, cov0, NN) - cov0 - cov1)
    k_x0 = eta * (proj0 - eta * exact_dot(cov1, proj0, NN))
    k_x1 = eta * proj1
    kwh, kwl = halves(k_w)
    kx = jnp.concatenate([k_x0, k_x1], axis=1)
    kxh, kxl = halves(kx)
    kx2 = jnp.concatenate([kxh, kxl], axis=0)
    kw2 = jnp.concatenate([kwh, kwl], axis=0)

    def unmixed(c):
        cut = slice(c * chunk, (c + 1) * chunk)
        part = fast_dot(kx2, x_ref[:, cut], NN) + fast_dot(kw2, whl_ref[0:rank, cut], NN)
        part = part[0:rank] + part[rank:2 * rank] + fast_dot(kwh, whl_ref[rank:2 * rank, cut], NN)
        m_ref[:, cut] = part

    for c in range(chunks):
        unmixed(c)
        advance(1)
    advance(len(pending))

    acc = jnp.zeros((2 * rank, rank), jnp.float32)
    outs = []
    for c in range(chunks):
        cut = slice(c * chunk, (c + 1) * chunk)
        ring[c, 2 * bits - 1].wait_recv()
        value = m_ref[:, cut] + av_ref[:, cut]
        m_ref[:, cut] = value
        copy = pltpu.make_async_copy(m_ref.at[:, cut], mixed_hbm.at[:, cut], out_sem.at[c])
        copy.start()
        outs.append(copy)
        mh, ml = halves(value)
        acc = acc + fast_dot(jnp.concatenate([mh, ml], axis=0), mh, NT)
    low_part = acc[rank:2 * rank]
    gram = (acc[0:rank] + (low_part + low_part.T)) / total_feat
    hr = rank // 2
    g_ref[...] = jnp.concatenate([gram[0:hr], gram[hr:rank]], axis=1)
    gc = remote(g_ref, g_core, core_send.at[2], core_recv.at[2], core_id)
    gc.wait_recv()
    g_sum[...] = g_ref[...] + g_core[...]
    g_copies = [
        remote(g_sum, g_recv.at[d], gz_send.at[d], gz_recv.at[d], z_ids[d]) for d in range(zs - 1)
    ]
    total = g_sum[...]
    for d in range(zs - 1):
        g_copies[d].wait_recv()
        total = total + g_recv[d]
    gram_ref[...] = total
    for copy in started + [gc] + g_copies + list(ring.values()):
        copy.wait_send()
    for copy in outs:
        copy.wait()


def solve_kernel(rank, cols, gram_ref, mixed_hbm, out_hbm, m_ref, o_ref, in_sem, out_sem):
    load = pltpu.make_async_copy(mixed_hbm, m_ref, in_sem.at[0])
    load.start()
    hr = rank // 2
    both = gram_ref[...]
    gram = jnp.concatenate([both[:, 0:rank], both[:, rank:2 * rank]], axis=0)
    eye = jnp.where(
        lax.broadcasted_iota(jnp.int32, (rank, rank), 0)
        == lax.broadcasted_iota(jnp.int32, (rank, rank), 1), 1.0, 0.0
    ).astype(jnp.float32)
    table = jnp.concatenate([gram, eye], axis=1)
    sub = 8
    blocks = [table[i * sub:(i + 1) * sub, :] for i in range(rank // sub)]
    ids = lax.broadcasted_iota(jnp.int32, (sub, 2 * rank), 0)
    for j in range(rank):
        b, r = divmod(j, sub)
        row = blocks[b][r:r + 1, :]
        inv = 1.0 / row[:, j:j + 1]
        scaled = row * inv
        for i in range(b, rank // sub):
            col = blocks[i][:, j:j + 1]
            update = col * scaled
            if i == b:
                update = jnp.where(ids > r, update, 0.0)
            blocks[i] = blocks[i] - update
    table = jnp.concatenate(blocks, axis=0)
    diag = jnp.sum(table[:, 0:rank] * eye, axis=1, keepdims=True)
    inverse = table[:, rank:2 * rank] * lax.rsqrt(diag)
    th, tl = halves(inverse)
    left = jnp.concatenate([th, th, tl], axis=1)
    load.wait()
    pieces = 4
    width = cols // pieces
    outs = []
    for p in range(pieces):
        cut = slice(p * width, (p + 1) * width)
        mh, ml = halves(m_ref[:, cut])
        o_ref[:, cut] = fast_dot(left, jnp.concatenate([mh, ml, mh], axis=0), NN)
        copy = pltpu.make_async_copy(o_ref.at[:, cut], out_hbm.at[:, cut], out_sem.at[p])
        copy.start()
        outs.append(copy)
    for copy in outs:
        copy.wait()


def per_device(basis, stream):
    reps = lax.axis_size("rep")
    feats = lax.axis_size("feat")
    start = basis[0]
    steps, rows, cols = stream.shape[1:]
    batches = stream[0].reshape(steps * rows, cols)
    rank = start.shape[0]
    bits = reps.bit_length() - 1
    chunk = LANE * reps
    chunks = cols // chunk
    zs = feats // 2
    half = rank + rows // 2
    f32 = jnp.float32
    vm = pltpu.VMEM
    hr = rank // 2
    dma = pltpu.SemaphoreType.DMA
    gram, mixed = pl.pallas_call(
        functools.partial(gather_kernel, reps, feats, rank, rows, cols, cols * feats),
        out_shape=(
            jax.ShapeDtypeStruct((hr, 2 * rank), f32),
            jax.ShapeDtypeStruct((rank, cols), f32),
        ),
        in_specs=[pl.BlockSpec(memory_space=pl.ANY)] * 2,
        out_specs=(pl.BlockSpec(memory_space=pltpu.VMEM), pl.BlockSpec(memory_space=pl.ANY)),
        scratch_shapes=[
            vm((rank, cols), f32),
            vm((steps * rows, cols), jnp.bfloat16),
            vm((2 * rank, cols), jnp.bfloat16),
            [vm((rank, cols >> (i + 1)), f32) for i in range(bits)],
            [vm((rank, cols >> (i + 1)), f32) for i in range(bits)],
            vm((rank, cols), f32),
            vm((rank, cols), f32),
            vm((2 * half, rows), f32),
            vm((half, rows), f32),
            vm((half, rows), f32),
            vm((zs - 1, half, rows), f32),
            vm((2 * half, rows), f32),
            vm((hr, 2 * rank), f32),
            vm((hr, 2 * rank), f32),
            vm((hr, 2 * rank), f32),
            vm((zs - 1, hr, 2 * rank), f32),
            dma((2,)),
            dma((chunks,)),
            dma((2 * bits, chunks)),
            dma((2 * bits, chunks)),
            dma((3,)),
            dma((3,)),
            dma((zs - 1,)),
            dma((zs - 1,)),
            dma((zs - 1,)),
            dma((zs - 1,)),
        ],
        compiler_params=pltpu.CompilerParams(collective_id=0, has_side_effects=True),
    )(start, batches)
    result = pl.pallas_call(
        functools.partial(solve_kernel, rank, cols),
        out_shape=jax.ShapeDtypeStruct((rank, cols), f32),
        in_specs=[pl.BlockSpec(memory_space=pltpu.VMEM), pl.BlockSpec(memory_space=pl.ANY)],
        out_specs=pl.BlockSpec(memory_space=pl.ANY),
        scratch_shapes=[vm((rank, cols), f32), vm((rank, cols), f32), dma((1,)), dma((4,))],
    )(gram, mixed)
    return result[None]


def solution(mesh):
    placed = (P("rep", None, "feat"), P("rep", None, None, "feat"))
    return jax.shard_map(
        per_device, mesh=mesh, in_specs=placed, out_specs=P("rep", None, "feat"), check_vma=False
    )
```

```python
import functools

import jax
import jax.numpy as jnp
from jax import lax
from jax.experimental import pallas as pl
from jax.experimental.pallas import tpu as pltpu
from jax.sharding import PartitionSpec as P

learn_rate = 0.5
LANE = 128
PLAN = (2, 18, 3, 1)
MESH = pl.DeviceIdType.MESH
NN = (((1,), (0,)), ((), ()))
NT = (((1,), (1,)), ((), ()))


def exact_dot(left, right, dims):
    return lax.dot_general(
        left, right, dims, precision=lax.Precision.HIGHEST, preferred_element_type=jnp.float32
    )


def fast_dot(left, right, dims):
    return lax.dot_general(left, right, dims, preferred_element_type=jnp.float32)


def halves(value):
    high = value.astype(jnp.bfloat16)
    low = (value - high.astype(jnp.float32)).astype(jnp.bfloat16)
    return high, low


def gather_kernel(
    reps, feats, rank, rows, cols, total_feat,
    basis_hbm, stream_hbm, gram_ref, mixed_hbm,
    w_ref, x_ref, whl_ref, sums_refs, recv_refs, av_ref, m_ref,
    pay_ref, half_recv, half_sum, z_recv, full_ref,
    g_ref, g_core, g_sum, g_recv,
    load_sem, out_sem, ring_send, ring_recv, core_send, core_recv, z_send, z_recv_sem,
    gz_send, gz_recv,
):
    bits = reps.bit_length() - 1
    chunk = LANE * reps
    chunks = cols // chunk
    zs = feats // 2
    me = lax.axis_index("rep")
    feat = lax.axis_index("feat")
    core = feat % 2
    zpos = feat // 2
    eta = learn_rate / rows
    scale = jnp.sqrt(jnp.float32(total_feat))

    load_w = pltpu.make_async_copy(basis_hbm, w_ref, load_sem.at[0])
    load_w.start()
    load_x = pltpu.make_async_copy(stream_hbm, x_ref, load_sem.at[1])
    load_x.start()

    def rep_peer(b):
        bit = (me // (1 << b)) % 2
        return me + (1 - 2 * bit) * (1 << b), bit

    rep_ids = [(rep_peer(b)[0], feat) for b in range(bits)]
    core_id = (me, feat + 1 - 2 * core)
    z_ids = [(me, ((zpos + d) % zs) * 2 + core) for d in range(1, zs)]

    barrier = pltpu.get_barrier_semaphore()
    for peer in rep_ids + [core_id] + z_ids:
        pl.semaphore_signal(barrier, inc=1, device_id=peer, device_id_type=MESH)
    pl.semaphore_wait(barrier, bits + 1 + zs - 1)
    load_w.wait()

    def remote(src, dst, send_sem, recv_sem, peer):
        copy = pltpu.make_async_remote_copy(
            src_ref=src, dst_ref=dst, send_sem=send_sem, recv_sem=recv_sem,
            device_id=peer, device_id_type=MESH,
        )
        copy.start()
        return copy

    started = []

    def at(off, width):
        return pl.ds(pl.multiple_of(off, LANE), width)

    def order(c):
        return [(c + i) % bits for i in range(bits)]

    keeps = []
    for c in range(chunks):
        off = c * chunk
        rec = []
        for i, b in enumerate(order(c)):
            width = chunk >> (i + 1)
            bit = rep_peer(b)[1]
            off = off + bit * width
            rec.append(off)
        keeps.append(rec)

    ring = {}

    def send_scatter(c, i):
        b = order(c)[i]
        width = chunk >> (i + 1)
        bit = rep_peer(b)[1]
        other = (1 - bit) * width
        if i == 0:
            src = w_ref.at[:, at(c * chunk + other, width)]
        else:
            src = sums_refs[i - 1].at[:, at(c * 2 * width + other, width)]
        dst = recv_refs[i].at[:, c * width:(c + 1) * width]
        ring[c, i] = remote(src, dst, ring_send.at[i, c], ring_recv.at[i, c], rep_ids[b])

    def take_scatter(c, i):
        b = order(c)[i]
        width = chunk >> (i + 1)
        bit = rep_peer(b)[1]
        ring[c, i].wait_recv()
        if i == 0:
            own = w_ref[:, at(c * chunk + bit * width, width)]
        else:
            own = sums_refs[i - 1][:, at(c * 2 * width + bit * width, width)]
        total = own + recv_refs[i][:, c * width:(c + 1) * width]
        if i == bits - 1:
            av_ref[:, at(keeps[c][i], width)] = total / reps
        else:
            sums_refs[i][:, c * width:(c + 1) * width] = total

    def send_gather(c, i):
        s = bits - 1 - i
        b = order(c)[s]
        width = chunk >> (s + 1)
        piece = av_ref.at[:, at(keeps[c][s], width)]
        k = bits + i
        ring[c, k] = remote(piece, piece, ring_send.at[k, c], ring_recv.at[k, c], rep_ids[b])

    for c in range(chunks):
        send_scatter(c, 0)

    def step(c, i):
        if i < bits:
            take_scatter(c, i)
        else:
            ring[c, i].wait_recv()
        if i + 1 < bits:
            send_scatter(c, i + 1)
        elif i + 1 < 2 * bits:
            send_gather(c, i + 1 - bits)

    pending = [(c, i) for i in range(2 * bits - 1) for c in range(chunks)]
    place = [0]

    def advance(count):
        for _ in range(count):
            if place[0] < len(pending):
                step(*pending[place[0]])
                place[0] += 1

    high, low = halves(w_ref[...])
    whl_ref[0:rank, :] = high
    whl_ref[rank:2 * rank, :] = low
    load_x.wait()
    x_all = x_ref[...]
    wx = fast_dot(whl_ref[...], x_all, NT)
    wx = wx[0:rank] + wx[rank:2 * rank]
    pay_ref[0:rank, :] = wx[:, 0:rows]
    pay_ref[rank:2 * rank, :] = wx[:, rows:2 * rows]
    pay_ref[2 * rank:2 * rank + rows, :] = fast_dot(x_ref[0:rows, :], x_ref[rows:2 * rows, :], NT)

    half = rank + rows // 2
    give = pl.ds(pl.multiple_of((1 - core) * half, 8), half)
    keep = pl.ds(pl.multiple_of(core * half, 8), half)
    core_copy = remote(pay_ref.at[give, :], half_recv, core_send.at[0], core_recv.at[0], core_id)
    advance(PLAN[0])
    core_copy.wait_recv()
    half_sum[...] = pay_ref[keep, :] + half_recv[...]
    z_copies = [
        remote(half_sum, z_recv.at[d], z_send.at[d], z_recv_sem.at[d], z_ids[d])
        for d in range(zs - 1)
    ]
    started.append(core_copy)
    started.extend(z_copies)
    advance(PLAN[1])
    total = half_sum[...]
    for d in range(zs - 1):
        z_copies[d].wait_recv()
        total = total + z_recv[d]
    full_ref[keep, :] = total
    share = remote(full_ref.at[keep, :], full_ref.at[keep, :], core_send.at[1], core_recv.at[1], core_id)
    started.append(share)
    advance(PLAN[2])
    share.wait_recv()

    first = full_ref[0:rank, :]
    second = full_ref[rank:2 * rank, :]
    cross = full_ref[2 * rank:2 * rank + rows, :]
    proj0 = first / scale
    cov0 = exact_dot(proj0, proj0, NT)
    drive1 = exact_dot(proj0, cross, NN)
    proj1 = (second + eta * (drive1 - exact_dot(cov0, second, NN))) / scale
    cov1 = exact_dot(proj1, proj1, NT)
    advance(PLAN[3])
    k_w = eta * (eta * exact_dot(cov1, cov0, NN) - cov0 - cov1)
    k_x0 = eta * (proj0 - eta * exact_dot(cov1, proj0, NN))
    k_x1 = eta * proj1
    kwh, kwl = halves(k_w)
    kx = jnp.concatenate([k_x0, k_x1], axis=1)
    kxh, kxl = halves(kx)
    kx2 = jnp.concatenate([kxh, kxl], axis=0)
    kw2 = jnp.concatenate([kwh, kwl], axis=0)

    def unmixed(c):
        cut = slice(c * chunk, (c + 1) * chunk)
        part = fast_dot(kx2, x_ref[:, cut], NN) + fast_dot(kw2, whl_ref[0:rank, cut], NN)
        part = part[0:rank] + part[rank:2 * rank] + fast_dot(kwh, whl_ref[rank:2 * rank, cut], NN)
        m_ref[:, cut] = part

    for c in range(chunks):
        unmixed(c)
        advance(1)
    advance(len(pending))

    acc = jnp.zeros((2 * rank, rank), jnp.float32)
    outs = []
    for c in range(chunks):
        cut = slice(c * chunk, (c + 1) * chunk)
        ring[c, 2 * bits - 1].wait_recv()
        value = m_ref[:, cut] + av_ref[:, cut]
        m_ref[:, cut] = value
        copy = pltpu.make_async_copy(m_ref.at[:, cut], mixed_hbm.at[:, cut], out_sem.at[c])
        copy.start()
        outs.append(copy)
        mh, ml = halves(value)
        acc = acc + fast_dot(jnp.concatenate([mh, ml], axis=0), mh, NT)
    low_part = acc[rank:2 * rank]
    gram = (acc[0:rank] + (low_part + low_part.T)) / total_feat
    hr = rank // 2
    g_ref[...] = jnp.concatenate([gram[0:hr], gram[hr:rank]], axis=1)
    gc = remote(g_ref, g_core, core_send.at[2], core_recv.at[2], core_id)
    gc.wait_recv()
    g_sum[...] = g_ref[...] + g_core[...]
    g_copies = [
        remote(g_sum, g_recv.at[d], gz_send.at[d], gz_recv.at[d], z_ids[d]) for d in range(zs - 1)
    ]
    total = g_sum[...]
    for d in range(zs - 1):
        g_copies[d].wait_recv()
        total = total + g_recv[d]
    gram_ref[...] = total
    for copy in started + [gc] + g_copies + list(ring.values()):
        copy.wait_send()
    for copy in outs:
        copy.wait()


def solve_kernel(rank, cols, gram_ref, mixed_hbm, out_hbm, m_ref, o_ref, in_sem, out_sem):
    load = pltpu.make_async_copy(mixed_hbm, m_ref, in_sem.at[0])
    load.start()
    hr = rank // 2
    both = gram_ref[...]
    gram = jnp.concatenate([both[:, 0:rank], both[:, rank:2 * rank]], axis=0)
    eye = jnp.where(
        lax.broadcasted_iota(jnp.int32, (rank, rank), 0)
        == lax.broadcasted_iota(jnp.int32, (rank, rank), 1), 1.0, 0.0
    ).astype(jnp.float32)
    table = jnp.concatenate([gram, eye], axis=1)
    sub = 8
    blocks = [table[i * sub:(i + 1) * sub, :] for i in range(rank // sub)]
    ids = lax.broadcasted_iota(jnp.int32, (sub, 2 * rank), 0)
    for j in range(0, rank, 4):
        b, r = divmod(j, sub)
        todo = range(b if r == 0 else b + 1, rank // sub)
        lanes = [jnp.broadcast_to(blocks[b][:, j + k:j + k + 1], (sub, 2 * rank)) for k in range(4)]
        cols4 = {
            i: [jnp.broadcast_to(blocks[i][:, j + k:j + k + 1], (sub, 2 * rank)) for k in range(4)]
            for i in todo if i != b
        }
        cols4[b] = lanes
        rows4 = [blocks[b][r + k:r + k + 1, :] for k in range(4)]
        d = [[lanes[l][r + k:r + k + 1, :] for l in range(4)] for k in range(4)]
        idet = 1.0 / (d[0][0] * d[1][1] - d[0][1] * d[1][0])
        i00, i01, i11 = d[1][1] * idet, -d[0][1] * idet, d[0][0] * idet
        y0 = i00 * rows4[0] + i01 * rows4[1]
        y1 = i01 * rows4[0] + i11 * rows4[1]
        y02, y12 = i00 * d[0][2] + i01 * d[1][2], i01 * d[0][2] + i11 * d[1][2]
        y03, y13 = i00 * d[0][3] + i01 * d[1][3], i01 * d[0][3] + i11 * d[1][3]
        e22 = d[2][2] - (d[2][0] * y02 + d[2][1] * y12)
        e23 = d[2][3] - (d[2][0] * y03 + d[2][1] * y13)
        e33 = d[3][3] - (d[3][0] * y03 + d[3][1] * y13)
        row2 = rows4[2] - (d[2][0] * y0 + d[2][1] * y1)
        row3 = rows4[3] - (d[3][0] * y0 + d[3][1] * y1)
        jdet = 1.0 / (e22 * e33 - e23 * e23)
        j00, j01, j11 = e33 * jdet, -e23 * jdet, e22 * jdet
        z0 = j00 * row2 + j01 * row3
        z1 = j01 * row2 + j11 * row3
        for i in todo:
            c = cols4[i]
            c2 = c[2] - (c[0] * y02 + c[1] * y12)
            c3 = c[3] - (c[0] * y03 + c[1] * y13)
            update = (c[0] * y0 + c[1] * y1) + (c2 * z0 + c3 * z1)
            if i == b:
                update = jnp.where(ids > r + 3, update, 0.0)
            blocks[i] = blocks[i] - update
        done = [
            rows4[0], rows4[1] - (d[0][1] / d[0][0]) * rows4[0],
            row2, row3 - (e23 / e22) * row2,
        ]
        block = blocks[b]
        for k in range(4):
            block = jnp.where(ids == r + k, done[k], block)
        blocks[b] = block
    table = jnp.concatenate(blocks, axis=0)
    diag = jnp.sum(table[:, 0:rank] * eye, axis=1, keepdims=True)
    inverse = table[:, rank:2 * rank] * lax.rsqrt(diag)
    th, tl = halves(inverse)
    left = jnp.concatenate([th, th, tl], axis=1)
    load.wait()
    pieces = 4
    width = cols // pieces
    outs = []
    for p in range(pieces):
        cut = slice(p * width, (p + 1) * width)
        mh, ml = halves(m_ref[:, cut])
        o_ref[:, cut] = fast_dot(left, jnp.concatenate([mh, ml, mh], axis=0), NN)
        copy = pltpu.make_async_copy(o_ref.at[:, cut], out_hbm.at[:, cut], out_sem.at[p])
        copy.start()
        outs.append(copy)
    for copy in outs:
        copy.wait()


def per_device(basis, stream):
    reps = lax.axis_size("rep")
    feats = lax.axis_size("feat")
    start = basis[0]
    steps, rows, cols = stream.shape[1:]
    batches = stream[0].reshape(steps * rows, cols)
    rank = start.shape[0]
    bits = reps.bit_length() - 1
    chunk = LANE * reps
    chunks = cols // chunk
    zs = feats // 2
    half = rank + rows // 2
    f32 = jnp.float32
    vm = pltpu.VMEM
    hr = rank // 2
    dma = pltpu.SemaphoreType.DMA
    gram, mixed = pl.pallas_call(
        functools.partial(gather_kernel, reps, feats, rank, rows, cols, cols * feats),
        out_shape=(
            jax.ShapeDtypeStruct((hr, 2 * rank), f32),
            jax.ShapeDtypeStruct((rank, cols), f32),
        ),
        in_specs=[pl.BlockSpec(memory_space=pl.ANY)] * 2,
        out_specs=(pl.BlockSpec(memory_space=pltpu.VMEM), pl.BlockSpec(memory_space=pl.ANY)),
        scratch_shapes=[
            vm((rank, cols), f32),
            vm((steps * rows, cols), jnp.bfloat16),
            vm((2 * rank, cols), jnp.bfloat16),
            [vm((rank, cols >> (i + 1)), f32) for i in range(bits)],
            [vm((rank, cols >> (i + 1)), f32) for i in range(bits)],
            vm((rank, cols), f32),
            vm((rank, cols), f32),
            vm((2 * half, rows), f32),
            vm((half, rows), f32),
            vm((half, rows), f32),
            vm((zs - 1, half, rows), f32),
            vm((2 * half, rows), f32),
            vm((hr, 2 * rank), f32),
            vm((hr, 2 * rank), f32),
            vm((hr, 2 * rank), f32),
            vm((zs - 1, hr, 2 * rank), f32),
            dma((2,)),
            dma((chunks,)),
            dma((2 * bits, chunks)),
            dma((2 * bits, chunks)),
            dma((3,)),
            dma((3,)),
            dma((zs - 1,)),
            dma((zs - 1,)),
            dma((zs - 1,)),
            dma((zs - 1,)),
        ],
        compiler_params=pltpu.CompilerParams(collective_id=0, has_side_effects=True),
    )(start, batches)
    result = pl.pallas_call(
        functools.partial(solve_kernel, rank, cols),
        out_shape=jax.ShapeDtypeStruct((rank, cols), f32),
        in_specs=[pl.BlockSpec(memory_space=pltpu.VMEM), pl.BlockSpec(memory_space=pl.ANY)],
        out_specs=pl.BlockSpec(memory_space=pl.ANY),
        scratch_shapes=[vm((rank, cols), f32), vm((rank, cols), f32), dma((1,)), dma((4,))],
    )(gram, mixed)
    return result[None]


def solution(mesh):
    placed = (P("rep", None, "feat"), P("rep", None, None, "feat"))
    return jax.shard_map(
        per_device, mesh=mesh, in_specs=placed, out_specs=P("rep", None, "feat"), check_vma=False
    )
```

```python
import functools

import jax
import jax.numpy as jnp
from jax import lax
from jax.experimental import pallas as pl
from jax.experimental.pallas import tpu as pltpu
from jax.sharding import PartitionSpec as P

learn_rate = 0.5
LANE = 128
PLAN = (2, 18, 3, 1)
MESH = pl.DeviceIdType.MESH
NN = (((1,), (0,)), ((), ()))
NT = (((1,), (1,)), ((), ()))


def exact_dot(left, right, dims):
    return lax.dot_general(
        left, right, dims, precision=lax.Precision.HIGHEST, preferred_element_type=jnp.float32
    )


def fast_dot(left, right, dims):
    return lax.dot_general(left, right, dims, preferred_element_type=jnp.float32)


def halves(value):
    high = value.astype(jnp.bfloat16)
    low = (value - high.astype(jnp.float32)).astype(jnp.bfloat16)
    return high, low


def gather_kernel(
    reps, feats, rank, rows, cols, total_feat,
    basis_hbm, stream_hbm, gram_ref, m_ref,
    w_ref, x_ref, whl_ref, sums_refs, recv_refs, av_ref,
    pay_ref, half_recv, half_sum, z_recv, full_ref,
    g_ref, g_core, g_sum, g_recv,
    load_sem, ring_send, ring_recv, core_send, core_recv, z_send, z_recv_sem,
    gz_send, gz_recv, hello_sem,
):
    bits = reps.bit_length() - 1
    chunk = LANE * reps
    chunks = cols // chunk
    zs = feats // 2
    me = lax.axis_index("rep")
    feat = lax.axis_index("feat")
    core = feat % 2
    zpos = feat // 2
    eta = learn_rate / rows
    scale = jnp.sqrt(jnp.float32(total_feat))

    loads = []
    for c in range(chunks):
        cut = slice(c * chunk, (c + 1) * chunk)
        loads.append(pltpu.make_async_copy(basis_hbm.at[:, cut], w_ref.at[:, cut], load_sem.at[c]))
        loads[c].start()
    load_x = pltpu.make_async_copy(stream_hbm, x_ref, load_sem.at[chunks])
    load_x.start()

    def rep_peer(b):
        bit = (me // (1 << b)) % 2
        return me + (1 - 2 * bit) * (1 << b), bit

    rep_ids = [(rep_peer(b)[0], feat) for b in range(bits)]
    core_id = (me, feat + 1 - 2 * core)
    z_ids = [(me, ((zpos + d) % zs) * 2 + core) for d in range(1, zs)]

    beside = (zpos > 0).astype(jnp.int32) + (zpos < zs - 1).astype(jnp.int32)

    def tell_beside(sem):
        for ahead, there in ((-1, zpos > 0), (1, zpos < zs - 1)):

            @pl.when(there)
            def _():
                pl.semaphore_signal(
                    sem, inc=1, device_id=(me, feat + 2 * ahead), device_id_type=MESH
                )

    barrier = pltpu.get_barrier_semaphore()
    for peer in rep_ids + [core_id]:
        pl.semaphore_signal(barrier, inc=1, device_id=peer, device_id_type=MESH)
    tell_beside(barrier)
    pl.semaphore_wait(barrier, bits + 1 + beside)

    def remote(src, dst, send_sem, recv_sem, peer):
        copy = pltpu.make_async_remote_copy(
            src_ref=src, dst_ref=dst, send_sem=send_sem, recv_sem=recv_sem,
            device_id=peer, device_id_type=MESH,
        )
        copy.start()
        return copy

    started = []

    def at(off, width):
        return pl.ds(pl.multiple_of(off, LANE), width)

    def order(c):
        return [(c + i) % bits for i in range(bits)]

    keeps = []
    for c in range(chunks):
        off = c * chunk
        rec = []
        for i, b in enumerate(order(c)):
            width = chunk >> (i + 1)
            bit = rep_peer(b)[1]
            off = off + bit * width
            rec.append(off)
        keeps.append(rec)

    ring = {}

    def send_scatter(c, i):
        b = order(c)[i]
        width = chunk >> (i + 1)
        bit = rep_peer(b)[1]
        other = (1 - bit) * width
        if i == 0:
            src = w_ref.at[:, at(c * chunk + other, width)]
        else:
            src = sums_refs[i - 1].at[:, at(c * 2 * width + other, width)]
        dst = recv_refs[i].at[:, c * width:(c + 1) * width]
        ring[c, i] = remote(src, dst, ring_send.at[i, c], ring_recv.at[i, c], rep_ids[b])

    def take_scatter(c, i):
        b = order(c)[i]
        width = chunk >> (i + 1)
        bit = rep_peer(b)[1]
        ring[c, i].wait_recv()
        if i == 0:
            own = w_ref[:, at(c * chunk + bit * width, width)]
        else:
            own = sums_refs[i - 1][:, at(c * 2 * width + bit * width, width)]
        total = own + recv_refs[i][:, c * width:(c + 1) * width]
        if i == bits - 1:
            av_ref[:, at(keeps[c][i], width)] = total / reps
        else:
            sums_refs[i][:, c * width:(c + 1) * width] = total

    def send_gather(c, i):
        s = bits - 1 - i
        b = order(c)[s]
        width = chunk >> (s + 1)
        piece = av_ref.at[:, at(keeps[c][s], width)]
        k = bits + i
        ring[c, k] = remote(piece, piece, ring_send.at[k, c], ring_recv.at[k, c], rep_ids[b])

    for c in range(chunks):
        loads[c].wait()
        send_scatter(c, 0)
    rounds = zs - 2
    if rounds > 0:
        tell_beside(hello_sem.at[0])

    def step(c, i):
        if i < bits:
            take_scatter(c, i)
        else:
            ring[c, i].wait_recv()
        if i + 1 < bits:
            send_scatter(c, i + 1)
        elif i + 1 < 2 * bits:
            send_gather(c, i + 1 - bits)

    pending = [(c, i) for i in range(2 * bits - 1) for c in range(chunks)]
    place = [0]

    def advance(count):
        for _ in range(count):
            if place[0] < len(pending):
                step(*pending[place[0]])
                place[0] += 1

    high, low = halves(w_ref[...])
    whl_ref[0:rank, :] = high
    whl_ref[rank:2 * rank, :] = low
    load_x.wait()
    x_all = x_ref[...]
    wx = fast_dot(whl_ref[...], x_all, NT)
    wx = wx[0:rank] + wx[rank:2 * rank]
    pay_ref[0:rank, :] = wx[:, 0:rows]
    pay_ref[rank:2 * rank, :] = wx[:, rows:2 * rows]
    pay_ref[2 * rank:2 * rank + rows, :] = fast_dot(x_ref[0:rows, :], x_ref[rows:2 * rows, :], NT)

    half = rank + rows // 2
    give = pl.ds(pl.multiple_of((1 - core) * half, 8), half)
    keep = pl.ds(pl.multiple_of(core * half, 8), half)
    core_copy = remote(pay_ref.at[give, :], half_recv, core_send.at[0], core_recv.at[0], core_id)
    advance(PLAN[0])
    core_copy.wait_recv()
    half_sum[...] = pay_ref[keep, :] + half_recv[...]
    for k in range(rounds):
        pl.semaphore_wait(hello_sem.at[k], beside)
        if k + 1 < rounds:
            tell_beside(hello_sem.at[k + 1])
    z_copies = [
        remote(half_sum, z_recv.at[d], z_send.at[d], z_recv_sem.at[d], z_ids[d])
        for d in range(zs - 1)
    ]
    started.append(core_copy)
    started.extend(z_copies)
    advance(PLAN[1])
    total = half_sum[...]
    for d in range(zs - 1):
        z_copies[d].wait_recv()
        total = total + z_recv[d]
    full_ref[keep, :] = total
    share = remote(full_ref.at[keep, :], full_ref.at[keep, :], core_send.at[1], core_recv.at[1], core_id)
    started.append(share)
    advance(PLAN[2])
    share.wait_recv()

    first = full_ref[0:rank, :]
    second = full_ref[rank:2 * rank, :]
    cross = full_ref[2 * rank:2 * rank + rows, :]
    proj0 = first / scale
    cov0 = exact_dot(proj0, proj0, NT)
    drive1 = exact_dot(proj0, cross, NN)
    proj1 = (second + eta * (drive1 - exact_dot(cov0, second, NN))) / scale
    cov1 = exact_dot(proj1, proj1, NT)
    advance(PLAN[3])
    k_w = eta * (eta * exact_dot(cov1, cov0, NN) - cov0 - cov1)
    k_x0 = eta * (proj0 - eta * exact_dot(cov1, proj0, NN))
    k_x1 = eta * proj1
    kwh, kwl = halves(k_w)
    kx = jnp.concatenate([k_x0, k_x1], axis=1)
    kxh, kxl = halves(kx)
    kx2 = jnp.concatenate([kxh, kxl], axis=0)
    kw2 = jnp.concatenate([kwh, kwl], axis=0)

    def unmixed(c):
        cut = slice(c * chunk, (c + 1) * chunk)
        part = fast_dot(kx2, x_ref[:, cut], NN) + fast_dot(kw2, whl_ref[0:rank, cut], NN)
        part = part[0:rank] + part[rank:2 * rank] + fast_dot(kwh, whl_ref[rank:2 * rank, cut], NN)
        m_ref[:, cut] = part

    for c in range(chunks):
        unmixed(c)
        advance(1)
    advance(len(pending))

    acc = jnp.zeros((2 * rank, rank), jnp.float32)
    for c in range(chunks):
        cut = slice(c * chunk, (c + 1) * chunk)
        ring[c, 2 * bits - 1].wait_recv()
        value = m_ref[:, cut] + av_ref[:, cut]
        m_ref[:, cut] = value
        mh, ml = halves(value)
        acc = acc + fast_dot(jnp.concatenate([mh, ml], axis=0), mh, NT)
    low_part = acc[rank:2 * rank]
    gram = (acc[0:rank] + (low_part + low_part.T)) / total_feat
    hr = rank // 2
    g_ref[...] = jnp.concatenate([gram[0:hr], gram[hr:rank]], axis=1)
    gc = remote(g_ref, g_core, core_send.at[2], core_recv.at[2], core_id)
    gc.wait_recv()
    g_sum[...] = g_ref[...] + g_core[...]
    g_copies = [
        remote(g_sum, g_recv.at[d], gz_send.at[d], gz_recv.at[d], z_ids[d]) for d in range(zs - 1)
    ]
    total = g_sum[...]
    for d in range(zs - 1):
        g_copies[d].wait_recv()
        total = total + g_recv[d]
    gram_ref[...] = total
    for copy in started + [gc] + g_copies + list(ring.values()):
        copy.wait_send()


def solve_kernel(rank, cols, gram_ref, m_ref, out_hbm, o_ref, out_sem):
    hr = rank // 2
    both = gram_ref[...]
    gram = jnp.concatenate([both[:, 0:rank], both[:, rank:2 * rank]], axis=0)
    eye = jnp.where(
        lax.broadcasted_iota(jnp.int32, (rank, rank), 0)
        == lax.broadcasted_iota(jnp.int32, (rank, rank), 1), 1.0, 0.0
    ).astype(jnp.float32)
    table = jnp.concatenate([gram, eye], axis=1)
    sub = 8
    blocks = [table[i * sub:(i + 1) * sub, :] for i in range(rank // sub)]
    ids = lax.broadcasted_iota(jnp.int32, (sub, 2 * rank), 0)
    for j in range(0, rank, 4):
        b, r = divmod(j, sub)
        todo = range(b if r == 0 else b + 1, rank // sub)
        lanes = [jnp.broadcast_to(blocks[b][:, j + k:j + k + 1], (sub, 2 * rank)) for k in range(4)]
        cols4 = {
            i: [jnp.broadcast_to(blocks[i][:, j + k:j + k + 1], (sub, 2 * rank)) for k in range(4)]
            for i in todo if i != b
        }
        cols4[b] = lanes
        rows4 = [blocks[b][r + k:r + k + 1, :] for k in range(4)]
        d = [[lanes[l][r + k:r + k + 1, :] for l in range(4)] for k in range(4)]
        idet = 1.0 / (d[0][0] * d[1][1] - d[0][1] * d[1][0])
        i00, i01, i11 = d[1][1] * idet, -d[0][1] * idet, d[0][0] * idet
        y0 = i00 * rows4[0] + i01 * rows4[1]
        y1 = i01 * rows4[0] + i11 * rows4[1]
        y02, y12 = i00 * d[0][2] + i01 * d[1][2], i01 * d[0][2] + i11 * d[1][2]
        y03, y13 = i00 * d[0][3] + i01 * d[1][3], i01 * d[0][3] + i11 * d[1][3]
        e22 = d[2][2] - (d[2][0] * y02 + d[2][1] * y12)
        e23 = d[2][3] - (d[2][0] * y03 + d[2][1] * y13)
        e33 = d[3][3] - (d[3][0] * y03 + d[3][1] * y13)
        row2 = rows4[2] - (d[2][0] * y0 + d[2][1] * y1)
        row3 = rows4[3] - (d[3][0] * y0 + d[3][1] * y1)
        jdet = 1.0 / (e22 * e33 - e23 * e23)
        j00, j01, j11 = e33 * jdet, -e23 * jdet, e22 * jdet
        z0 = j00 * row2 + j01 * row3
        z1 = j01 * row2 + j11 * row3
        for i in todo:
            c = cols4[i]
            c2 = c[2] - (c[0] * y02 + c[1] * y12)
            c3 = c[3] - (c[0] * y03 + c[1] * y13)
            update = (c[0] * y0 + c[1] * y1) + (c2 * z0 + c3 * z1)
            if i == b:
                update = jnp.where(ids > r + 3, update, 0.0)
            blocks[i] = blocks[i] - update
        done = [
            rows4[0], rows4[1] - (d[0][1] / d[0][0]) * rows4[0],
            row2, row3 - (e23 / e22) * row2,
        ]
        block = blocks[b]
        for k in range(4):
            block = jnp.where(ids == r + k, done[k], block)
        blocks[b] = block
    table = jnp.concatenate(blocks, axis=0)
    diag = jnp.sum(table[:, 0:rank] * eye, axis=1, keepdims=True)
    inverse = table[:, rank:2 * rank] * lax.rsqrt(diag)
    th, tl = halves(inverse)
    left = jnp.concatenate([th, th, tl], axis=1)
    pieces = 4
    width = cols // pieces
    outs = []
    for p in range(pieces):
        cut = slice(p * width, (p + 1) * width)
        mh, ml = halves(m_ref[:, cut])
        o_ref[:, cut] = fast_dot(left, jnp.concatenate([mh, ml, mh], axis=0), NN)
        copy = pltpu.make_async_copy(o_ref.at[:, cut], out_hbm.at[:, cut], out_sem.at[p])
        copy.start()
        outs.append(copy)
    for copy in outs:
        copy.wait()


def per_device(basis, stream):
    reps = lax.axis_size("rep")
    feats = lax.axis_size("feat")
    start = basis[0]
    steps, rows, cols = stream.shape[1:]
    batches = stream[0].reshape(steps * rows, cols)
    rank = start.shape[0]
    bits = reps.bit_length() - 1
    chunk = LANE * reps
    chunks = cols // chunk
    zs = feats // 2
    half = rank + rows // 2
    f32 = jnp.float32
    vm = pltpu.VMEM
    hr = rank // 2
    dma = pltpu.SemaphoreType.DMA
    gram, mixed = pl.pallas_call(
        functools.partial(gather_kernel, reps, feats, rank, rows, cols, cols * feats),
        out_shape=(
            pltpu.VMEM((hr, 2 * rank), f32),
            pltpu.VMEM((rank, cols), f32),
        ),
        in_specs=[pl.BlockSpec(memory_space=pl.ANY)] * 2,
        out_specs=(pl.BlockSpec(memory_space=pltpu.VMEM), pl.BlockSpec(memory_space=pltpu.VMEM)),
        scratch_shapes=[
            vm((rank, cols), f32),
            vm((steps * rows, cols), jnp.bfloat16),
            vm((2 * rank, cols), jnp.bfloat16),
            [vm((rank, cols >> (i + 1)), f32) for i in range(bits)],
            [vm((rank, cols >> (i + 1)), f32) for i in range(bits)],
            vm((rank, cols), f32),
            vm((2 * half, rows), f32),
            vm((half, rows), f32),
            vm((half, rows), f32),
            vm((zs - 1, half, rows), f32),
            vm((2 * half, rows), f32),
            vm((hr, 2 * rank), f32),
            vm((hr, 2 * rank), f32),
            vm((hr, 2 * rank), f32),
            vm((zs - 1, hr, 2 * rank), f32),
            dma((chunks + 1,)),
            dma((2 * bits, chunks)),
            dma((2 * bits, chunks)),
            dma((3,)),
            dma((3,)),
            dma((zs - 1,)),
            dma((zs - 1,)),
            dma((zs - 1,)),
            dma((zs - 1,)),
            pltpu.SemaphoreType.REGULAR((max(zs - 2, 1),)),
        ],
        compiler_params=pltpu.CompilerParams(collective_id=0, has_side_effects=True),
    )(start, batches)
    result = pl.pallas_call(
        functools.partial(solve_kernel, rank, cols),
        out_shape=jax.ShapeDtypeStruct((rank, cols), f32),
        in_specs=[pl.BlockSpec(memory_space=pltpu.VMEM)] * 2,
        out_specs=pl.BlockSpec(memory_space=pl.ANY),
        scratch_shapes=[vm((rank, cols), f32), dma((4,))],
    )(
        pltpu.with_memory_space_constraint(gram, pltpu.VMEM),
        pltpu.with_memory_space_constraint(mixed, pltpu.VMEM),
    )
    return result[None]


def solution(mesh):
    placed = (P("rep", None, "feat"), P("rep", None, None, "feat"))
    return jax.shard_map(
        per_device, mesh=mesh, in_specs=placed, out_specs=P("rep", None, "feat"), check_vma=False
    )
```

```python
import functools

import jax
import jax.numpy as jnp
from jax import lax
from jax.experimental import pallas as pl
from jax.experimental.pallas import tpu as pltpu
from jax.sharding import PartitionSpec as P

learn_rate = 0.5
LANE = 128
PLAN = (2, 18, 3, 1)
MESH = pl.DeviceIdType.MESH
NN = (((1,), (0,)), ((), ()))
NT = (((1,), (1,)), ((), ()))


def exact_dot(left, right, dims):
    return lax.dot_general(
        left, right, dims, precision=lax.Precision.HIGHEST, preferred_element_type=jnp.float32
    )


def fast_dot(left, right, dims):
    return lax.dot_general(left, right, dims, preferred_element_type=jnp.float32)


def halves(value):
    high = value.astype(jnp.bfloat16)
    low = (value - high.astype(jnp.float32)).astype(jnp.bfloat16)
    return high, low


def gather_kernel(
    reps, feats, rank, rows, cols, total_feat,
    basis_hbm, stream_hbm, gram_ref, m_ref,
    w_ref, x_ref, whl_ref, sums_refs, recv_refs, av_ref,
    pay_ref, half_recv, half_sum, z_recv, full_ref,
    g_ref, g_core, g_sum, g_recv,
    load_sem, ring_send, ring_recv, core_send, core_recv, z_send, z_recv_sem,
    gz_send, gz_recv, hello_sem,
):
    bits = reps.bit_length() - 1
    chunk = LANE * reps
    chunks = cols // chunk
    zs = feats // 2
    me = lax.axis_index("rep")
    feat = lax.axis_index("feat")
    core = feat % 2
    zpos = feat // 2
    eta = learn_rate / rows
    scale = jnp.sqrt(jnp.float32(total_feat))

    loads = []
    for c in range(chunks):
        cut = slice(c * chunk, (c + 1) * chunk)
        loads.append(pltpu.make_async_copy(basis_hbm.at[:, cut], w_ref.at[:, cut], load_sem.at[c]))
        loads[c].start()
    load_x = pltpu.make_async_copy(stream_hbm, x_ref, load_sem.at[chunks])
    load_x.start()

    def rep_peer(b):
        bit = (me // (1 << b)) % 2
        return me + (1 - 2 * bit) * (1 << b), bit

    rep_ids = [(rep_peer(b)[0], feat) for b in range(bits)]
    core_id = (me, feat + 1 - 2 * core)
    z_ids = [(me, ((zpos + d) % zs) * 2 + core) for d in range(1, zs)]

    beside = (zpos > 0).astype(jnp.int32) + (zpos < zs - 1).astype(jnp.int32)

    def tell_beside(sem):
        for ahead, there in ((-1, zpos > 0), (1, zpos < zs - 1)):

            @pl.when(there)
            def _():
                pl.semaphore_signal(
                    sem, inc=1, device_id=(me, feat + 2 * ahead), device_id_type=MESH
                )

    barrier = pltpu.get_barrier_semaphore()
    for peer in rep_ids + [core_id]:
        pl.semaphore_signal(barrier, inc=1, device_id=peer, device_id_type=MESH)
    tell_beside(barrier)
    pl.semaphore_wait(barrier, bits + 1 + beside)

    def remote(src, dst, send_sem, recv_sem, peer):
        copy = pltpu.make_async_remote_copy(
            src_ref=src, dst_ref=dst, send_sem=send_sem, recv_sem=recv_sem,
            device_id=peer, device_id_type=MESH,
        )
        copy.start()
        return copy

    started = []

    def at(off, width):
        return pl.ds(pl.multiple_of(off, LANE), width)

    def order(c):
        return [(c + i) % bits for i in range(bits)]

    keeps = []
    for c in range(chunks):
        off = c * chunk
        rec = []
        for i, b in enumerate(order(c)):
            width = chunk >> (i + 1)
            bit = rep_peer(b)[1]
            off = off + bit * width
            rec.append(off)
        keeps.append(rec)

    ring = {}

    def send_scatter(c, i):
        b = order(c)[i]
        width = chunk >> (i + 1)
        bit = rep_peer(b)[1]
        other = (1 - bit) * width
        if i == 0:
            src = w_ref.at[:, at(c * chunk + other, width)]
        else:
            src = sums_refs[i - 1].at[:, at(c * 2 * width + other, width)]
        dst = recv_refs[i].at[:, c * width:(c + 1) * width]
        ring[c, i] = remote(src, dst, ring_send.at[i, c], ring_recv.at[i, c], rep_ids[b])

    def take_scatter(c, i):
        b = order(c)[i]
        width = chunk >> (i + 1)
        bit = rep_peer(b)[1]
        ring[c, i].wait_recv()
        if i == 0:
            own = w_ref[:, at(c * chunk + bit * width, width)]
        else:
            own = sums_refs[i - 1][:, at(c * 2 * width + bit * width, width)]
        total = own + recv_refs[i][:, c * width:(c + 1) * width]
        if i == bits - 1:
            av_ref[:, at(keeps[c][i], width)] = total / reps
        else:
            sums_refs[i][:, c * width:(c + 1) * width] = total

    def send_gather(c, i):
        s = bits - 1 - i
        b = order(c)[s]
        width = chunk >> (s + 1)
        piece = av_ref.at[:, at(keeps[c][s], width)]
        k = bits + i
        ring[c, k] = remote(piece, piece, ring_send.at[k, c], ring_recv.at[k, c], rep_ids[b])

    for c in range(chunks):
        loads[c].wait()
        send_scatter(c, 0)
    rounds = zs - 2
    if rounds > 0:
        tell_beside(hello_sem.at[0])

    def step(c, i):
        if i < bits:
            take_scatter(c, i)
        else:
            ring[c, i].wait_recv()
        if i + 1 < bits:
            send_scatter(c, i + 1)
        elif i + 1 < 2 * bits:
            send_gather(c, i + 1 - bits)

    pending = [(c, i) for i in range(2 * bits - 1) for c in range(chunks)]
    place = [0]

    def advance(count):
        for _ in range(count):
            if place[0] < len(pending):
                step(*pending[place[0]])
                place[0] += 1

    high, low = halves(w_ref[...])
    whl_ref[0:rank, :] = high
    whl_ref[rank:2 * rank, :] = low
    load_x.wait()
    x_all = x_ref[...]
    wx = fast_dot(whl_ref[...], x_all, NT)
    wx = wx[0:rank] + wx[rank:2 * rank]
    pay_ref[0:rank, :] = wx[:, 0:rows]
    pay_ref[rank:2 * rank, :] = wx[:, rows:2 * rows]
    pay_ref[2 * rank:2 * rank + rows, :] = fast_dot(x_ref[0:rows, :], x_ref[rows:2 * rows, :], NT)

    half = rank + rows // 2
    give = pl.ds(pl.multiple_of((1 - core) * half, 8), half)
    keep = pl.ds(pl.multiple_of(core * half, 8), half)
    core_copy = remote(pay_ref.at[give, :], half_recv, core_send.at[0], core_recv.at[0], core_id)
    advance(PLAN[0])
    core_copy.wait_recv()
    half_sum[...] = pay_ref[keep, :] + half_recv[...]
    for k in range(rounds):
        pl.semaphore_wait(hello_sem.at[k], beside)
        if k + 1 < rounds:
            tell_beside(hello_sem.at[k + 1])
    z_copies = [
        remote(half_sum, z_recv.at[d], z_send.at[d], z_recv_sem.at[d], z_ids[d])
        for d in range(zs - 1)
    ]
    started.append(core_copy)
    started.extend(z_copies)
    advance(PLAN[1])
    total = half_sum[...]
    for d in range(zs - 1):
        z_copies[d].wait_recv()
        total = total + z_recv[d]
    full_ref[keep, :] = total
    share = remote(full_ref.at[keep, :], full_ref.at[keep, :], core_send.at[1], core_recv.at[1], core_id)
    started.append(share)
    advance(PLAN[2])
    share.wait_recv()

    first = full_ref[0:rank, :]
    second = full_ref[rank:2 * rank, :]
    cross = full_ref[2 * rank:2 * rank + rows, :]
    proj0 = first / scale
    cov0 = exact_dot(proj0, proj0, NT)
    drive1 = exact_dot(proj0, cross, NN)
    proj1 = (second + eta * (drive1 - exact_dot(cov0, second, NN))) / scale
    cov1 = exact_dot(proj1, proj1, NT)
    advance(PLAN[3])
    k_w = eta * (eta * exact_dot(cov1, cov0, NN) - cov0 - cov1)
    k_x0 = eta * (proj0 - eta * exact_dot(cov1, proj0, NN))
    k_x1 = eta * proj1
    kwh, kwl = halves(k_w)
    kx = jnp.concatenate([k_x0, k_x1], axis=1)
    kxh, kxl = halves(kx)
    kx2 = jnp.concatenate([kxh, kxl], axis=0)
    kw2 = jnp.concatenate([kwh, kwl], axis=0)

    def unmixed(c):
        cut = slice(c * chunk, (c + 1) * chunk)
        part = fast_dot(kx2, x_ref[:, cut], NN) + fast_dot(kw2, whl_ref[0:rank, cut], NN)
        part = part[0:rank] + part[rank:2 * rank] + fast_dot(kwh, whl_ref[rank:2 * rank, cut], NN)
        m_ref[:, cut] = part

    for c in range(chunks):
        unmixed(c)
        advance(1)
    advance(len(pending))

    acc = [jnp.zeros((2 * rank, rank), jnp.float32)]

    def mix(off, width):
        cut = at(off, width)
        value = m_ref[:, cut] + av_ref[:, cut]
        m_ref[:, cut] = value
        mh, ml = halves(value)
        acc[0] = acc[0] + fast_dot(jnp.concatenate([mh, ml], axis=0), mh, NT)

    wide = chunk // 2
    for c in range(chunks):
        mix(keeps[c][0], wide)
    for c in range(chunks):
        ring[c, 2 * bits - 1].wait_recv()
        mix(2 * c * chunk + wide - keeps[c][0], wide)
    acc = acc[0]
    low_part = acc[rank:2 * rank]
    gram = (acc[0:rank] + (low_part + low_part.T)) / total_feat
    hr = rank // 2
    g_ref[...] = jnp.concatenate([gram[0:hr], gram[hr:rank]], axis=1)
    gc = remote(g_ref, g_core, core_send.at[2], core_recv.at[2], core_id)
    gc.wait_recv()
    g_sum[...] = g_ref[...] + g_core[...]
    g_copies = [
        remote(g_sum, g_recv.at[d], gz_send.at[d], gz_recv.at[d], z_ids[d]) for d in range(zs - 1)
    ]
    total = g_sum[...]
    for d in range(zs - 1):
        g_copies[d].wait_recv()
        total = total + g_recv[d]
    gram_ref[...] = total
    for copy in started + [gc] + g_copies + list(ring.values()):
        copy.wait_send()


def solve_kernel(rank, cols, gram_ref, m_ref, out_hbm, o_ref, out_sem):
    hr = rank // 2
    both = gram_ref[...]
    gram = jnp.concatenate([both[:, 0:rank], both[:, rank:2 * rank]], axis=0)
    eye = jnp.where(
        lax.broadcasted_iota(jnp.int32, (rank, rank), 0)
        == lax.broadcasted_iota(jnp.int32, (rank, rank), 1), 1.0, 0.0
    ).astype(jnp.float32)
    table = jnp.concatenate([gram, eye], axis=1)
    sub = 8
    blocks = [table[i * sub:(i + 1) * sub, :] for i in range(rank // sub)]
    ids = lax.broadcasted_iota(jnp.int32, (sub, 2 * rank), 0)
    pieces = 4
    width = cols // pieces
    outs = []

    def finish(lo, hi):
        part = jnp.concatenate(blocks[lo // sub:hi // sub], axis=0)
        diag = jnp.sum(part[:, 0:rank] * eye[lo:hi], axis=1, keepdims=True)
        th, tl = halves(part[:, rank:rank + hi] * lax.rsqrt(diag))
        left = jnp.concatenate([th, th, tl], axis=1)
        for p in range(pieces):
            cut = slice(p * width, (p + 1) * width)
            mh, ml = halves(m_ref[0:hi, cut])
            o_ref[lo:hi, cut] = fast_dot(left, jnp.concatenate([mh, ml, mh], axis=0), NN)
            copy = pltpu.make_async_copy(
                o_ref.at[lo:hi, cut], out_hbm.at[lo:hi, cut], out_sem.at[len(outs)]
            )
            copy.start()
            outs.append(copy)

    for j in range(0, rank, 4):
        if j == hr:
            finish(0, hr)
        b, r = divmod(j, sub)
        todo = range(b if r == 0 else b + 1, rank // sub)
        lanes = [jnp.broadcast_to(blocks[b][:, j + k:j + k + 1], (sub, 2 * rank)) for k in range(4)]
        cols4 = {
            i: [jnp.broadcast_to(blocks[i][:, j + k:j + k + 1], (sub, 2 * rank)) for k in range(4)]
            for i in todo if i != b
        }
        cols4[b] = lanes
        rows4 = [blocks[b][r + k:r + k + 1, :] for k in range(4)]
        d = [[lanes[l][r + k:r + k + 1, :] for l in range(4)] for k in range(4)]
        idet = 1.0 / (d[0][0] * d[1][1] - d[0][1] * d[1][0])
        i00, i01, i11 = d[1][1] * idet, -d[0][1] * idet, d[0][0] * idet
        y0 = i00 * rows4[0] + i01 * rows4[1]
        y1 = i01 * rows4[0] + i11 * rows4[1]
        y02, y12 = i00 * d[0][2] + i01 * d[1][2], i01 * d[0][2] + i11 * d[1][2]
        y03, y13 = i00 * d[0][3] + i01 * d[1][3], i01 * d[0][3] + i11 * d[1][3]
        e22 = d[2][2] - (d[2][0] * y02 + d[2][1] * y12)
        e23 = d[2][3] - (d[2][0] * y03 + d[2][1] * y13)
        e33 = d[3][3] - (d[3][0] * y03 + d[3][1] * y13)
        row2 = rows4[2] - (d[2][0] * y0 + d[2][1] * y1)
        row3 = rows4[3] - (d[3][0] * y0 + d[3][1] * y1)
        jdet = 1.0 / (e22 * e33 - e23 * e23)
        j00, j01, j11 = e33 * jdet, -e23 * jdet, e22 * jdet
        z0 = j00 * row2 + j01 * row3
        z1 = j01 * row2 + j11 * row3
        for i in todo:
            c = cols4[i]
            c2 = c[2] - (c[0] * y02 + c[1] * y12)
            c3 = c[3] - (c[0] * y03 + c[1] * y13)
            update = (c[0] * y0 + c[1] * y1) + (c2 * z0 + c3 * z1)
            if i == b:
                update = jnp.where(ids > r + 3, update, 0.0)
            blocks[i] = blocks[i] - update
        done = [
            rows4[0], rows4[1] - (d[0][1] / d[0][0]) * rows4[0],
            row2, row3 - (e23 / e22) * row2,
        ]
        block = blocks[b]
        for k in range(4):
            block = jnp.where(ids == r + k, done[k], block)
        blocks[b] = block
    finish(hr, rank)
    for copy in outs:
        copy.wait()


def per_device(basis, stream):
    reps = lax.axis_size("rep")
    feats = lax.axis_size("feat")
    start = basis[0]
    steps, rows, cols = stream.shape[1:]
    batches = stream[0].reshape(steps * rows, cols)
    rank = start.shape[0]
    bits = reps.bit_length() - 1
    chunk = LANE * reps
    chunks = cols // chunk
    zs = feats // 2
    half = rank + rows // 2
    f32 = jnp.float32
    vm = pltpu.VMEM
    hr = rank // 2
    dma = pltpu.SemaphoreType.DMA
    gram, mixed = pl.pallas_call(
        functools.partial(gather_kernel, reps, feats, rank, rows, cols, cols * feats),
        out_shape=(
            pltpu.VMEM((hr, 2 * rank), f32),
            pltpu.VMEM((rank, cols), f32),
        ),
        in_specs=[pl.BlockSpec(memory_space=pl.ANY)] * 2,
        out_specs=(pl.BlockSpec(memory_space=pltpu.VMEM), pl.BlockSpec(memory_space=pltpu.VMEM)),
        scratch_shapes=[
            vm((rank, cols), f32),
            vm((steps * rows, cols), jnp.bfloat16),
            vm((2 * rank, cols), jnp.bfloat16),
            [vm((rank, cols >> (i + 1)), f32) for i in range(bits)],
            [vm((rank, cols >> (i + 1)), f32) for i in range(bits)],
            vm((rank, cols), f32),
            vm((2 * half, rows), f32),
            vm((half, rows), f32),
            vm((half, rows), f32),
            vm((zs - 1, half, rows), f32),
            vm((2 * half, rows), f32),
            vm((hr, 2 * rank), f32),
            vm((hr, 2 * rank), f32),
            vm((hr, 2 * rank), f32),
            vm((zs - 1, hr, 2 * rank), f32),
            dma((chunks + 1,)),
            dma((2 * bits, chunks)),
            dma((2 * bits, chunks)),
            dma((3,)),
            dma((3,)),
            dma((zs - 1,)),
            dma((zs - 1,)),
            dma((zs - 1,)),
            dma((zs - 1,)),
            pltpu.SemaphoreType.REGULAR((max(zs - 2, 1),)),
        ],
        compiler_params=pltpu.CompilerParams(collective_id=0, has_side_effects=True),
    )(start, batches)
    result = pl.pallas_call(
        functools.partial(solve_kernel, rank, cols),
        out_shape=jax.ShapeDtypeStruct((rank, cols), f32),
        in_specs=[pl.BlockSpec(memory_space=pltpu.VMEM)] * 2,
        out_specs=pl.BlockSpec(memory_space=pl.ANY),
        scratch_shapes=[vm((rank, cols), f32), dma((8,))],
    )(
        pltpu.with_memory_space_constraint(gram, pltpu.VMEM),
        pltpu.with_memory_space_constraint(mixed, pltpu.VMEM),
    )
    return result[None]


def solution(mesh):
    placed = (P("rep", None, "feat"), P("rep", None, None, "feat"))
    return jax.shard_map(
        per_device, mesh=mesh, in_specs=placed, out_specs=P("rep", None, "feat"), check_vma=False
    )
```
